32 devices in a mesh: tm: 2 (over y), space: 4 (over z), member: 4 (over x, core).
Axes of the slice: x: 2, y: 2, z: 4, core: 2. Of those that a mesh axis runs over, the one named last changes fastest.
Arguments:
- obs_anom: bfloat16 [6, 2, 8, 256, 1024], P('tm', None, 'space', 'member'), may hold values from -0.59375 to 0.59375
- obs_prec: bfloat16 [6, 2, 8, 1024], P('tm', None, 'space'), may hold values from 0.29882812 to 3
- innov: bfloat16 [6, 2, 8, 1024], P('tm', None, 'space'), may hold values from -6 to 6
- obs_column: int32 [6, 2, 8, 1024], P('tm', None, 'space'), may hold values from 0 to 127
- cutoff: int32 [2, 8], replicated, may hold values from 1 to 2
- inv_root: float32 [2, 8, 256, 256], P('tm', 'space'), may hold values from -0.12 to 0.12
- state_anom: bfloat16 [2, 8, 256, 32, 128], P('tm', 'space', None, 'member'), may hold values from -6 to 6
- state_mean: float32 [2, 8, 32, 128], P('tm', 'space', 'member'), may hold values from -6 to 6
Outputs:
- analysis: bfloat16 [2, 8, 256, 32, 128], P('tm', 'space', None, 'member')
The draws below stay inside these ranges and needn't reach their ends.
All inputs are finite; a program needn't handle non-finite values.
Results may differ from the reference program's by a relative error of at most 0.0062.
Values may be sent and summed in bfloat16 or wider, within the bound.
A program may use at most 64 MiB of HBM per device.

```python
import math
import jax
import jax.numpy as jnp
from jax import lax

K = 256
SLOTS = 6
OBS = 1024
HALO = 2
LEVELS = 32
POINTS = 128
NEWTON = 2
SECTORS = 2
TILES_SEC = 8


def common_factor(key):
    return jax.random.uniform(jax.random.fold_in(key, 11), (K,), jnp.float32, -2.0, 2.0)


def draw_obs_anom(key, part):
    extent = (SLOTS, SECTORS, TILES_SEC, K, OBS)
    code_extent = (SLOTS, SECTORS, TILES_SEC, 1, OBS)
    spread = 3.8 / math.sqrt(OBS)
    factor = common_factor(key)
    noise_key = jax.random.fold_in(key, 3)
    code_key = jax.random.fold_in(key, 5)
    share = 0.3
    noise_draw = jax.random.truncated_normal(noise_key, -3.0, 3.0, extent, jnp.float32)
    codes = jax.random.truncated_normal(code_key, -2.0, 2.0, code_extent, jnp.float32)
    values = math.sqrt(1.0 - share) * noise_draw + math.sqrt(share) * factor[:, None] * codes
    return (values * spread).astype(jnp.bfloat16)


def draw_inv_root(key, part):
    extent = (SECTORS, TILES_SEC, K, K)
    spread = 0.1 / math.sqrt(K)
    total = 108.0 * (HALO / 2 + 1)
    factor = common_factor(key)
    direction = factor / jnp.sqrt(jnp.sum(factor * factor))
    noise_key = jax.random.fold_in(key, 7)
    share = 0.3
    noise_draw = jax.random.truncated_normal(noise_key, -4.0, 4.0, extent, jnp.float32)
    centre = 1.0 / math.sqrt(K - 1 + total * (1.0 - share))
    along = 1.0 / jnp.sqrt(K - 1 + total * (1.0 - share + share * jnp.sum(factor * factor)))
    symmetric = (noise_draw + jnp.swapaxes(noise_draw, -1, -2)) * (spread / math.sqrt(2.0))
    identity = jnp.eye(K, dtype=jnp.float32)
    outer_dir = direction[:, None] * direction[None, :]
    project = identity - outer_dir
    symmetric = jnp.einsum('ij,stjk,kl->stil', project, symmetric, project, precision=jax.lax.Precision.HIGHEST)
    result = centre * (identity + symmetric) + (along - centre) * outer_dir
    return result.astype(jnp.float32)


def touch_ends(values, stream_key, low, high):
    longest = values.shape.index(max(values.shape))
    spots = []
    for shift in (0, 1):
        where = [jax.random.randint(jax.random.fold_in(stream_key, axis), (), 0, length) for axis, length in enumerate(values.shape)]
        where[longest] = (where[longest] + shift) % values.shape[longest]
        spots.append(tuple(where))
    return values.at[spots[0]].set(low).at[spots[1]].set(high)


def shard_levels(own_key, shape, cuts, least, top_value):
    def one(axis_at, blocks):
        draws = jax.random.uniform(jax.random.fold_in(jax.random.fold_in(own_key, 6), axis_at), (blocks,), jnp.float32, least / len(cuts), top_value / len(cuts))
        return jnp.repeat(jnp.exp(draws), shape[axis_at] // blocks).reshape((-1,) + (1,) * (len(shape) - axis_at - 1))

    level = one(*cuts[0])
    for cut in cuts[1:]:
        level = level * one(*cut)
    return level


def scatter_about(own_key, shape, deviation, bound, shards=(), kind=jnp.bfloat16):
    values = jax.random.normal(own_key, shape, jnp.float32) * deviation
    if len(shards) > 0:
        values = shard_levels(own_key, shape, shards, -0.22, 0.18) * values
    return jnp.clip(values, min=-bound, max=bound).astype(kind)


def setup_inputs(seed: int = 0) -> dict:
    key_list = jax.random.split(jax.random.key(seed), 9)
    return {
        "obs_anom": draw_obs_anom(jax.random.fold_in(key_list[8], 71), 0),
        "obs_prec": jnp.clip(jnp.exp(math.log(3.0) - 2.306499 * jax.random.uniform(key_list[1], (SLOTS, SECTORS, TILES_SEC, OBS), jnp.float32) ** shard_levels(key_list[1], (SLOTS, SECTORS, TILES_SEC, OBS), ((0, 2), (2, 4)), -0.2, 0.2)), 0.29882812, 3.0).astype(jnp.bfloat16),
        "innov": scatter_about(key_list[2], (SLOTS, SECTORS, TILES_SEC, OBS), 1.0, 6.0, ((0, 2), (2, 4))),
        "obs_column": touch_ends(jax.random.randint(key_list[3], (SLOTS, SECTORS, TILES_SEC, OBS), 0, POINTS), jax.random.fold_in(key_list[3], 1), 0, POINTS - 1).astype(jnp.int32),
        "cutoff": touch_ends(jax.random.randint(key_list[4], (SECTORS, TILES_SEC), 1, HALO + 1), jax.random.fold_in(key_list[4], 1), 1, HALO).astype(jnp.int32),
        "inv_root": draw_inv_root(jax.random.fold_in(key_list[8], 71), 0),
        "state_anom": scatter_about(key_list[6], (SECTORS, TILES_SEC, K, LEVELS, POINTS), 1.0, 6.0, ((0, 2), (1, 4), (3, 4))),
        "state_mean": scatter_about(key_list[7], (SECTORS, TILES_SEC, LEVELS, POINTS), 1.0, 6.0, ((0, 2), (1, 4), (2, 4)), jnp.float32),
    }


def taper_weight(distance, reach_now, columns):
    scaled_reach = (reach_now + 0.5) * columns
    relative = distance / scaled_reach
    return jnp.square(jnp.maximum(1.0 - relative * relative, 0.0))

def reference(obs_anom, obs_prec, innov, obs_column, cutoff, inv_root, state_anom, state_mean):
    tile_total = SECTORS * TILES_SEC
    anomaly = obs_anom.reshape(SLOTS, tile_total, K, OBS)
    precision = obs_prec.reshape(SLOTS, tile_total, OBS).astype(jnp.float32)
    innovation = innov.reshape(SLOTS, tile_total, OBS).astype(jnp.float32)
    placing = obs_column.reshape(SLOTS, tile_total, OBS).astype(jnp.float32) + (0.5 - POINTS / 2)
    reaches = cutoff.reshape(tile_total).astype(jnp.float32)
    root_all = inv_root.reshape(tile_total, K, K)
    anomalies = state_anom.reshape(tile_total, K, LEVELS * POINTS)
    mean_rows = state_mean.reshape(tile_total, 1, LEVELS * POINTS)
    offsets = jnp.arange(-HALO, HALO + 1, dtype=jnp.int32)
    shifts = offsets.astype(jnp.float32)
    identity = jnp.eye(K, dtype=jnp.float32)
    highest = lax.Precision.HIGHEST

    def analyse(tile_index):
        beside_all = (tile_index + offsets + tile_total) % tile_total
        window = jnp.take(anomaly, beside_all, axis=1)
        window_prec = jnp.take(precision, beside_all, axis=1)
        window_innov = jnp.take(innovation, beside_all, axis=1)
        window_place = jnp.take(placing, beside_all, axis=1)
        distance = shifts[None, :, None] * POINTS + window_place
        coeffs = taper_weight(distance, reaches[tile_index], POINTS) * window_prec
        scaled = (window.astype(jnp.float32) * coeffs[:, :, None, :]).astype(jnp.bfloat16)
        weighted = (coeffs * window_innov).astype(jnp.bfloat16)
        gram_part = jnp.einsum('swko,swlo->kl', scaled.astype(jnp.float32), window.astype(jnp.float32))
        proj_part = jnp.einsum('swko,swo->k', window.astype(jnp.float32), weighted.astype(jnp.float32))
        system = (K - 1.0) * identity + gram_part
        inv_sqrt = root_all[tile_index]
        for newton_step in range(NEWTON):
            square = jnp.dot(inv_sqrt, inv_sqrt, precision=highest)
            applied = jnp.dot(system, square, precision=highest)
            inv_sqrt = 1.5 * inv_sqrt - 0.5 * jnp.dot(inv_sqrt, applied, precision=highest)
        mean_weight = jnp.dot(inv_sqrt, jnp.dot(inv_sqrt, proj_part, precision=highest), precision=highest)
        weights = (mean_weight[:, None] + math.sqrt(K - 1) * inv_sqrt).astype(jnp.bfloat16)
        result = mean_rows[tile_index] + jnp.dot(weights.T, anomalies[tile_index], preferred_element_type=jnp.float32)
        return result.astype(jnp.bfloat16)
    analysis = lax.map(analyse, jnp.arange(tile_total, dtype=jnp.int32))
    return analysis.reshape(SECTORS, TILES_SEC, K, LEVELS, POINTS)
```

```python
import functools
import math

import jax
import jax.numpy as jnp
from jax import lax
from jax.experimental import pallas as pl
from jax.experimental.pallas import tpu as pltpu
from jax.sharding import PartitionSpec as P

HALO = 2
NEWTON = 2
WINDOW = 2 * HALO + 1
PAD = 16
MESH = pl.DeviceIdType.MESH
F32 = jnp.float32
BF16 = jnp.bfloat16


def split(x):
    hi = x.astype(BF16)
    return hi, (x - hi.astype(F32)).astype(BF16)


def dot_nn(a, b):
    return jnp.dot(a, b, preferred_element_type=F32)


def dot_nt(a, b):
    return lax.dot_general(a, b, (((1,), (1,)), ((), ())), preferred_element_type=F32)


def dot3(a, b, dot):
    ah, al = a
    bh, bl = b
    return dot(ah, bh) + (dot(ah, bl) + dot(al, bh))


def kernel(
    groups,
    spaces,
    parts,
    columns,
    obs_ref,
    prec_ref,
    innov_ref,
    column_ref,
    cut_ref,
    root_hbm,
    mean_hbm,
    out_ref,
    flat_ref,
    held,
    roots,
    means_in,
    recv,
    prec,
    innov,
    column,
    lhs,
    gram,
    proj,
    square,
    core_out,
    core_in,
    core_proj,
    halo_out,
    halo_in,
    halo_proj_out,
    halo_proj,
    far_out,
    far_in,
    far_proj_out,
    far_proj,
    back_out,
    back_in,
    send_sem,
    recv_sem,
    own_sem,
    local_sem,
    info_sem,
    pair_send,
    pair_recv,
):
    slots, _, tiles, share, obs = obs_ref.shape
    members = share * parts
    quarter = obs // parts
    block = members // 2
    half = block // 2
    extended = tiles + 2 * HALO
    g = lax.axis_index("tm")
    z = lax.axis_index("space")
    m = lax.axis_index("member")
    ring = groups * spaces
    place = g * spaces + z
    right = lax.rem(place + 1, ring)
    left = lax.rem(place + ring - 1, ring)

    def ring_id(index):
        return {"tm": lax.div(index, spaces), "space": lax.rem(index, spaces)}

    peers = [(dt, dm) for dt in range(groups) for dm in range(parts) if dt or dm]
    peers.sort(key=lambda p: (-(p[0] + (p[1] > 0)), p[1]))

    def peer_id(dt, dm):
        return {"tm": lax.rem(g + dt, groups), "member": lax.rem(m + dm, parts)}

    core_bit = lax.rem(m, 2)
    core_id = {"member": m + 1 - 2 * core_bit}
    span = parts // 2
    far_id = {"member": lax.rem(m + span, parts)}

    barrier = pltpu.get_barrier_semaphore()
    for side in (left, right):
        pl.semaphore_signal(barrier, inc=1, device_id=ring_id(side), device_id_type=MESH)
    for dt, dm in peers:
        pl.semaphore_signal(barrier, inc=1, device_id=peer_id(dt, dm), device_id_type=MESH)

    def own_copy(c):
        return pltpu.make_async_copy(
            obs_ref.at[c, g, :, :, pl.ds(pl.multiple_of(m * quarter, quarter), quarter)],
            recv.at[
                c,
                :,
                pl.ds(pl.multiple_of(m * share, share), share),
                pl.ds(pl.multiple_of(g * quarter, quarter), quarter),
            ],
            own_sem.at[c],
        )

    quarter_mine = pl.ds(pl.multiple_of(m * quarter, quarter), quarter)
    quarter_group = pl.ds(pl.multiple_of(g * quarter, quarter), quarter)
    vectors = [(prec_ref, prec), (innov_ref, innov), (column_ref, column)]

    def own_info():
        return [
            pltpu.make_async_copy(
                src.at[:, g, :, quarter_mine], dst.at[:, :, quarter_group], info_sem.at[0, n]
            )
            for n, (src, dst) in enumerate(vectors)
        ]

    def info_copy(dt):
        other = lax.rem(g + dt, groups)
        return [
            pltpu.make_async_remote_copy(
                src_ref=src.at[:, other, :, quarter_mine],
                dst_ref=dst.at[:, :, quarter_group],
                send_sem=info_sem.at[2 * dt - 1, n],
                recv_sem=info_sem.at[2 * dt, n],
                device_id={"tm": other},
                device_id_type=MESH,
            )
            for n, (src, dst) in enumerate(vectors)
        ]

    def obs_copy(c, slot, dt, dm):
        to_m = lax.rem(m + dm, parts)
        return pltpu.make_async_remote_copy(
            src_ref=held.at[
                c,
                lax.rem(g + dt, groups),
                :,
                :,
                pl.ds(pl.multiple_of(to_m * quarter, quarter), quarter),
            ],
            dst_ref=recv.at[
                c,
                :,
                pl.ds(pl.multiple_of(m * share, share), share),
                pl.ds(pl.multiple_of(g * quarter, quarter), quarter),
            ],
            send_sem=send_sem.at[c, slot],
            recv_sem=recv_sem.at[c, slot],
            device_id=peer_id(dt, dm),
            device_id_type=MESH,
        )

    held_copies = [
        pltpu.make_async_copy(obs_ref.at[c], held.at[c], local_sem.at[c]) for c in range(slots)
    ]
    root_copy = pltpu.make_async_copy(root_hbm.at[0], roots, local_sem.at[slots])
    mean_copy = pltpu.make_async_copy(mean_hbm.at[0], means_in, local_sem.at[slots + 1])
    for copy in held_copies:
        copy.start()
    for copy in own_info():
        copy.start()
    root_copy.start()
    mean_copy.start()
    for c in range(slots):
        own_copy(c).start()
    pl.semaphore_wait(barrier, len(peers) + 2)
    for dt in range(1, groups):
        for copy in info_copy(dt):
            copy.start()
    for c in range(slots):
        held_copies[c].wait()
        for slot, (dt, dm) in enumerate(peers):
            obs_copy(c, slot, dt, dm).start()

    gram[...] = jnp.zeros_like(gram)
    proj[...] = jnp.zeros_like(proj)
    root_copy.wait()
    mean_copy.wait()
    levels = means_in.shape[1]
    for t in range(tiles):
        for level in range(levels):
            flat_ref[t : t + 1, level * columns : (level + 1) * columns] = means_in[
                t, level : level + 1
            ]
        x = split(roots[t])
        square[t] = dot3(x, x, dot_nn)

    per_sector = cut_ref.shape[1]
    cycle = cut_ref.shape[0] * per_sector
    first = place * tiles
    reaches = []
    for e in range(extended):
        at = lax.rem(first + e - HALO + cycle, cycle)
        reach = cut_ref[lax.div(at, per_sector), lax.rem(at, per_sector)]
        reaches.append((reach.astype(F32) + 0.5) * columns)

    for copy in own_info():
        copy.wait()
    for dt in range(1, groups):
        for copy in info_copy(dt):
            copy.wait()

    wide = groups * quarter
    row = lax.broadcasted_iota(jnp.int32, (PAD, wide), 0)
    shift = (HALO - row).astype(F32) * columns

    def add_chunk(c, carry):
        own_copy(c).wait()
        for slot, (dt, dm) in enumerate(peers):
            obs_copy(c, slot, dt, dm).wait_recv()
        all_precision = prec[c].astype(F32)
        all_innovation = innov[c].astype(F32)
        all_placing = column[c].astype(F32) + (0.5 - columns / 2)
        for u in range(tiles):
            precision = all_precision[u : u + 1]
            innovation = all_innovation[u : u + 1]
            placing = all_placing[u : u + 1]
            reach = jnp.ones((PAD, wide), F32)
            for w in range(WINDOW):
                reach = jnp.where(row == w, reaches[u + w], reach)
            relative = (shift + placing) / reach
            taper = jnp.square(jnp.maximum(1.0 - relative * relative, 0.0))
            coeffs = jnp.where(row < WINDOW, taper * precision, 0.0)
            anomaly = recv[c, u]
            wide_anomaly = anomaly.astype(F32)
            for w in range(WINDOW):
                lhs[w * members : (w + 1) * members] = (
                    wide_anomaly * coeffs[w : w + 1]
                ).astype(BF16)
            lhs[WINDOW * members :] = (coeffs * innovation).astype(BF16)
            sums = dot_nt(lhs[...], anomaly)
            for w in range(WINDOW):
                gram[u + w] += sums[w * members : (w + 1) * members]
            base = WINDOW * members
            proj[u : u + WINDOW, :members] += sums[base : base + WINDOW]
        return carry

    lax.fori_loop(0, slots, add_chunk, 0)

    def remote(src, dst, index, target):
        return pltpu.make_async_remote_copy(
            src_ref=src,
            dst_ref=dst,
            send_sem=pair_send.at[index],
            recv_sem=pair_recv.at[index],
            device_id=target,
            device_id_type=MESH,
        )

    rows = lax.broadcasted_iota(jnp.int32, (block, block), 0)
    cols = lax.broadcasted_iota(jnp.int32, (block, block), 1)
    for e in range(extended):
        corner = gram[e, block:, block:]
        diagonal = jnp.sum(jnp.where(rows == cols, corner, 0.0), axis=0, keepdims=True)
        proj[e : e + 1, members:] = diagonal
        gram[e, :block, :block] = jnp.where(rows <= cols, gram[e, :block, :block], corner)

    mine = pl.multiple_of(core_bit * half, half)
    theirs = pl.multiple_of((1 - core_bit) * half, half)

    core_out[...] = gram[:, pl.ds(theirs, half)].astype(BF16)
    core_copies = [
        remote(core_out, core_in, 0, core_id),
        remote(proj, core_proj, 1, core_id),
    ]
    for copy in core_copies:
        copy.start()
    for copy in core_copies:
        copy.wait()

    summed = proj[...] + core_proj[...]
    halo_proj_out[...] = jnp.zeros_like(halo_proj_out)
    far_proj_out[...] = jnp.zeros_like(far_proj_out)
    pieces_of = summed.shape[1] // block

    def pack(target, first_row, count):
        for h in range(count):
            for k in range(pieces_of):
                at = h * pieces_of + k
                target[at : at + 1] = summed[
                    first_row + h : first_row + h + 1, k * block : (k + 1) * block
                ]

    pack(halo_proj_out.at[0], 0, HALO)
    pack(halo_proj_out.at[1], tiles + HALO, HALO)
    pack(far_proj_out, HALO, tiles)
    low = gram[:HALO, pl.ds(mine, half)] + core_in[:HALO].astype(F32)
    halo_out[0] = low.astype(BF16)
    high = gram[tiles + HALO :, pl.ds(mine, half)] + core_in[tiles + HALO :].astype(F32)
    halo_out[1] = high.astype(BF16)
    halo_copies = [
        remote(halo_out.at[0], halo_in.at[0], 2, ring_id(left)),
        remote(halo_out.at[1], halo_in.at[1], 3, ring_id(right)),
        remote(halo_proj_out.at[0], halo_proj.at[0], 4, ring_id(left)),
        remote(halo_proj_out.at[1], halo_proj.at[1], 5, ring_id(right)),
    ]
    for copy in halo_copies:
        copy.start()
    owned = [
        gram[HALO + t, pl.ds(mine, half)] + core_in[HALO + t].astype(F32) for t in range(tiles)
    ]
    for copy in halo_copies:
        copy.wait()
    strip = HALO * pieces_of
    start = (tiles - HALO) * pieces_of
    far_proj_out[:strip] += halo_proj[1, :strip]
    far_proj_out[start : start + strip] += halo_proj[0, :strip]
    for h in range(HALO):
        owned[h] = owned[h] + halo_in[1, h].astype(F32)
        t = tiles - HALO + h
        owned[t] = owned[t] + halo_in[0, h].astype(F32)

    for t in range(tiles):
        far_out[t] = owned[t].astype(BF16)
        gram[t, pl.ds(mine, half)] = owned[t]
    far_copies = [
        remote(far_out, far_in, 6, far_id),
        remote(far_proj_out, far_proj, 7, far_id),
    ]
    for copy in far_copies:
        copy.start()
    for copy in far_copies:
        copy.wait()

    for t in range(tiles):
        total = gram[t, pl.ds(mine, half)] + far_in[t].astype(F32)
        gram[t, pl.ds(mine, half)] = total
        back_out[t] = total.astype(BF16)
    back_copy = remote(back_out, back_in, 8, core_id)
    back_copy.start()
    back_copy.wait()
    for t in range(tiles):
        gram[t, pl.ds(theirs, half)] = back_in[t].astype(F32)

    packed_proj = far_proj_out[...] + far_proj[...]
    for t in range(tiles):
        for k in range(pieces_of):
            at = t * pieces_of + k
            proj[t : t + 1, k * block : (k + 1) * block] = packed_proj[at : at + 1]
    total_proj = proj[...]
    inflation = members - 1.0
    eye = jnp.where(
        lax.broadcasted_iota(jnp.int32, (members, members), 0)
        == lax.broadcasted_iota(jnp.int32, (members, members), 1),
        1.0,
        0.0,
    )
    systems = []
    for t in range(tiles):
        packed = gram[t, :block, :block]
        flipped = packed.T
        cross = gram[t, :block, block:]
        gram[t, :block, :block] = jnp.where(rows <= cols, packed, flipped)
        corner = jnp.where(rows > cols, packed, flipped)
        gram[t, block:, block:] = jnp.where(rows == cols, total_proj[t : t + 1, members:], corner)
        gram[t, block:, :block] = cross.T
        systems.append(split(gram[t] + inflation * eye))
    xs = [roots[t] for t in range(tiles)]
    for step in range(NEWTON):
        pieces = [split(x) for x in xs]
        if step == 0:
            powers = [square[t] for t in range(tiles)]
        else:
            powers = [dot3(piece, piece, dot_nn) for piece in pieces]
        powers = [split(power) for power in powers]
        applied = [dot3(system, power, dot_nn) for system, power in zip(systems, powers)]
        excess = [(a - eye).astype(BF16) for a in applied]
        xs = [x - 0.5 * dot_nn(piece[0], d) for x, piece, d in zip(xs, pieces, excess)]
    pieces = [split(x) for x in xs]
    totals = split(total_proj[:, :members])
    inner = [dot3(piece, totals, dot_nt) for piece in pieces]
    means = [dot3(piece, split(part), dot_nn) for piece, part in zip(pieces, inner)]
    for t in range(tiles):
        out_ref[t] = (means[t][:, t : t + 1] + math.sqrt(inflation) * xs[t]).astype(BF16)

    def drain(c, carry):
        for slot, (dt, dm) in enumerate(peers):
            obs_copy(c, slot, dt, dm).wait_send()
        return carry

    lax.fori_loop(0, slots, drain, 0)


def body(mesh_shape, obs_anom, obs_prec, innov, obs_column, cutoff, inv_root, state_anom, state_mean):
    groups, spaces, parts = (mesh_shape[name] for name in ("tm", "space", "member"))
    slots, _, tiles, share, obs = obs_anom.shape
    columns = state_anom.shape[-1]
    members = share * parts
    quarter = obs // parts
    half = members // 4
    long = members + members // 2
    extended = tiles + 2 * HALO
    halo_rows = -(-3 * HALO // 8) * 8
    far_rows = -(-3 * tiles // 8) * 8
    vmem = pl.BlockSpec(memory_space=pltpu.VMEM)
    hbm = pl.BlockSpec(memory_space=pl.ANY)
    peers = groups * parts - 1
    levels = state_mean.shape[2]
    weights, flat = pl.pallas_call(
        functools.partial(kernel, groups, spaces, parts, columns),
        out_shape=[
            jax.ShapeDtypeStruct((tiles, members, members), BF16),
            jax.ShapeDtypeStruct((tiles, levels * columns), F32),
        ],
        in_specs=[hbm, hbm, hbm, hbm, pl.BlockSpec(memory_space=pltpu.SMEM), hbm, hbm],
        out_specs=[vmem, vmem],
        scratch_shapes=[
            pltpu.VMEM(obs_anom.shape, BF16),
            pltpu.VMEM((tiles, members, members), F32),
            pltpu.VMEM((tiles, levels, columns), F32),
            pltpu.VMEM((slots, tiles, members, groups * quarter), BF16),
            pltpu.VMEM((slots, tiles, groups * quarter), BF16),
            pltpu.VMEM((slots, tiles, groups * quarter), BF16),
            pltpu.VMEM((slots, tiles, groups * quarter), jnp.int32),
            pltpu.VMEM((WINDOW * members + PAD, groups * quarter), BF16),
            pltpu.VMEM((extended, members, members), F32),
            pltpu.VMEM((8, long), F32),
            pltpu.VMEM((tiles, members, members), F32),
            pltpu.VMEM((extended, half, members), BF16),
            pltpu.VMEM((extended, half, members), BF16),
            pltpu.VMEM((8, long), F32),
            pltpu.VMEM((2, HALO, half, members), BF16),
            pltpu.VMEM((2, HALO, half, members), BF16),
            pltpu.VMEM((2, halo_rows, members // 2), F32),
            pltpu.VMEM((2, halo_rows, members // 2), F32),
            pltpu.VMEM((tiles, half, members), BF16),
            pltpu.VMEM((tiles, half, members), BF16),
            pltpu.VMEM((far_rows, members // 2), F32),
            pltpu.VMEM((far_rows, members // 2), F32),
            pltpu.VMEM((tiles, half, members), BF16),
            pltpu.VMEM((tiles, half, members), BF16),
            pltpu.SemaphoreType.DMA((slots, peers)),
            pltpu.SemaphoreType.DMA((slots, peers)),
            pltpu.SemaphoreType.DMA((slots,)),
            pltpu.SemaphoreType.DMA((slots + 2,)),
            pltpu.SemaphoreType.DMA((2 * groups - 1, 3)),
            pltpu.SemaphoreType.DMA((9,)),
            pltpu.SemaphoreType.DMA((9,)),
        ],
        compiler_params=pltpu.CompilerParams(collective_id=0, has_side_effects=True),
    )(obs_anom, obs_prec, innov, obs_column, cutoff, inv_root, state_mean)
    anomalies = state_anom[0].reshape(tiles, members, -1)
    mean_rows = flat[:, None, :]
    result = (
        jnp.einsum("tij,tiq->tjq", weights, anomalies, preferred_element_type=F32) + mean_rows
    )
    return result.astype(BF16).reshape(state_anom.shape)


def solution(mesh):
    in_specs = (
        P("tm", None, "space", "member", None),
        P("tm", None, "space", None),
        P("tm", None, "space", None),
        P("tm", None, "space", None),
        P(),
        P("tm", "space", None, None),
        P("tm", "space", None, "member", None),
        P("tm", "space", "member", None),
    )
    out_specs = P("tm", "space", None, "member", None)
    step = functools.partial(body, dict(mesh.shape))
    return jax.shard_map(step, mesh=mesh, in_specs=in_specs, out_specs=out_specs, check_vma=False)
```
